32 devices in a mesh: dp: 8 (over z, y), ep: 4 (over x, core).
Axes of the slice: x: 2, y: 2, z: 4, core: 2. Of those that a mesh axis runs over, the one named last changes fastest.
Arguments:
- tokens: bfloat16 [65536, 768], P(('dp', 'ep'))
- out_grad: bfloat16 [65536, 768], P(('dp', 'ep'))
- routes: int32 [65536, 2], P(('dp', 'ep'))
- norm_gain: float32 [768], replicated
- w_router: float32 [768, 8], replicated
- w_gate: bfloat16 [8, 768, 3072], P('ep')
- w_up: bfloat16 [8, 768, 3072], P('ep')
- w_down: bfloat16 [8, 3072, 768], P('ep')
Outputs:
- output 1: bfloat16 [65536, 768], P(('dp', 'ep'))
- output 2: bfloat16 [65536, 768], P(('dp', 'ep'))
- output 3: float32 [768], replicated
- output 4: float32 [768, 8], replicated
- output 5: bfloat16 [8, 768, 3072], P('ep')
- output 6: bfloat16 [8, 768, 3072], P('ep')
- output 7: bfloat16 [8, 3072, 768], P('ep')
All inputs are finite; a program needn't handle non-finite values.
Results may differ from the reference program's by a relative error of at most 0.0136066.
Values are sent between devices in bfloat16 or wider.
A program may use at most 1 GiB of HBM per device.

```python
import jax
import jax.numpy as jnp
from jax import lax

D = 768
FF = 3072
EXPERTS = 8
TOKENS = 2048
DEV_COUNT = 32
CAPACITY = 640
NORM_EPS = 1e-5
ALL_ROWS = DEV_COUNT * TOKENS
ALL_SLOTS = EXPERTS * CAPACITY


def draw_routes(rng_key):
    hot_key, first_key, second_key = jax.random.split(rng_key, 3)
    offset_table = jnp.array([0, 0, 0, 0, 0, 0, 0, 0, 0, 0, 1, 1, 1, 1, 1, 1, 2, 2, 2, 3, 3, 3, 4, 4, 4, 5, 5, 5, 6, 6, 7, 7], jnp.int32)
    hot_expert = jax.random.randint(hot_key, (DEV_COUNT, 1), 0, EXPERTS)
    draw_ids = jax.random.randint(first_key, (DEV_COUNT, TOKENS), 0, 32)
    first_pick = (hot_expert + offset_table[draw_ids]) % EXPERTS
    second_pick = (first_pick + 1 + jax.random.randint(second_key, (DEV_COUNT, TOKENS), 0, EXPERTS - 1)) % EXPERTS
    return jnp.stack([first_pick, second_pick], axis=-1).reshape(ALL_ROWS, 2).astype(jnp.int32)


def setup_inputs(seed: int = 0) -> dict:
    key_list = jax.random.split(jax.random.key(seed), 8)
    tokens = jax.random.normal(key_list[0], (ALL_ROWS, D), jnp.float32).astype(jnp.bfloat16)
    out_grad = jax.random.normal(key_list[1], (ALL_ROWS, D), jnp.float32).astype(jnp.bfloat16)
    routes = draw_routes(key_list[2])
    norm_gain = jax.random.uniform(key_list[3], (D,), jnp.float32, 0.5, 1.5)
    w_router = jax.random.normal(key_list[4], (D, EXPERTS), jnp.float32) * D ** -0.5
    w_gate = (jax.random.normal(key_list[5], (EXPERTS, D, FF), jnp.float32) * D ** -0.5).astype(jnp.bfloat16)
    w_up = (jax.random.normal(key_list[6], (EXPERTS, D, FF), jnp.float32) * D ** -0.5).astype(jnp.bfloat16)
    w_down = (jax.random.normal(key_list[7], (EXPERTS, FF, D), jnp.float32) * FF ** -0.5).astype(jnp.bfloat16)
    return {'tokens': tokens, 'out_grad': out_grad, 'routes': routes, 'norm_gain': norm_gain, 'w_router': w_router, 'w_gate': w_gate, 'w_up': w_up, 'w_down': w_down}


def slot_table(route_dev):
    expert_ids = jnp.arange(EXPERTS, dtype=jnp.int32)
    first_hot = (route_dev[:, :, 0:1] == expert_ids).astype(jnp.int32)
    second_hot = (route_dev[:, :, 1:2] == expert_ids).astype(jnp.int32)
    first_run = jnp.cumsum(first_hot, axis=1)
    second_run = jnp.cumsum(second_hot, axis=1) + first_run[:, -1:, :]
    first_pos = jnp.sum((first_run - 1) * first_hot, axis=-1)
    second_pos = jnp.sum((second_run - 1) * second_hot, axis=-1)
    positions = jnp.stack([first_pos, second_pos], axis=-1)
    return jnp.where(positions < CAPACITY, route_dev * CAPACITY + positions, ALL_SLOTS)


def slot_owner(slot_ids):
    token_ids = jnp.broadcast_to(jnp.arange(TOKENS, dtype=jnp.int32)[:, None], (TOKENS, 2))
    owner_ids = jnp.full((ALL_SLOTS + 1,), TOKENS, jnp.int32).at[slot_ids.reshape(-1)].set(token_ids.reshape(-1))
    return owner_ids[:ALL_SLOTS]


def gather_rows(source_rows, row_ids):
    return jnp.take(source_rows, row_ids, axis=0)


batched_rows = jax.vmap(gather_rows)


def expert_body(operands):
    slot_rows, gate_w, up_w, down_w = operands
    gate_act = jnp.dot(slot_rows, gate_w, preferred_element_type=jnp.float32)
    up_act = jnp.dot(slot_rows, up_w, preferred_element_type=jnp.float32)
    hidden = (jax.nn.silu(gate_act) * up_act).astype(jnp.bfloat16)
    return jnp.dot(hidden, down_w, preferred_element_type=jnp.float32).astype(jnp.bfloat16)


expert_mlp = jax.checkpoint(expert_body)


def reference(tokens, out_grad, routes, norm_gain, w_router, w_gate, w_up, w_down):
    route_dev = routes.reshape(DEV_COUNT, TOKENS, 2)
    slot_ids = slot_table(route_dev)
    owner_ids = jax.vmap(slot_owner)(slot_ids)
    pick_ids = slot_ids.reshape(DEV_COUNT, TOKENS * 2)

    def moe_block(tokens, norm_gain, w_router, w_gate, w_up, w_down):
        x_f32 = tokens.reshape(DEV_COUNT, TOKENS, D).astype(jnp.float32)
        inv_rms = lax.rsqrt(jnp.mean(x_f32 * x_f32, axis=-1, keepdims=True) + NORM_EPS)
        normed = (x_f32 * inv_rms * norm_gain).astype(jnp.bfloat16)
        logits = jnp.einsum('ntd,de->nte', normed.astype(jnp.float32), w_router)
        gate_probs = jax.nn.softmax(jnp.take_along_axis(logits, route_dev, axis=-1), axis=-1)
        padded = jnp.concatenate([normed, jnp.zeros_like(normed[:, :1])], axis=1)
        send_rows = batched_rows(padded, owner_ids)
        expert_rows = send_rows.reshape(DEV_COUNT, EXPERTS, CAPACITY, D).transpose(1, 0, 2, 3).reshape(EXPERTS, DEV_COUNT * CAPACITY, D)
        expert_out = lax.map(expert_mlp, (expert_rows, w_gate, w_up, w_down))
        back_rows = expert_out.reshape(EXPERTS, DEV_COUNT, CAPACITY, D).transpose(1, 0, 2, 3).reshape(DEV_COUNT, ALL_SLOTS, D)
        back_rows = jnp.concatenate([back_rows, jnp.zeros_like(back_rows[:, :1])], axis=1)
        picked = batched_rows(back_rows, pick_ids).reshape(DEV_COUNT, TOKENS, 2, D).astype(jnp.float32)
        mixed_rows = x_f32 + jnp.sum(gate_probs[..., None] * picked, axis=2)
        return mixed_rows.astype(jnp.bfloat16).reshape(ALL_ROWS, D)

    block_out, pullback = jax.vjp(moe_block, tokens, norm_gain, w_router, w_gate, w_up, w_down)
    grad_list = pullback(out_grad)
    return (block_out, grad_list[0], grad_list[1], grad_list[2], grad_list[3], grad_list[4], grad_list[5])
```

```python
import jax
import jax.numpy as jnp
from jax import lax
from jax.sharding import PartitionSpec as P

CAPACITY_NUM = 5
CAPACITY_DEN = 4
NORM_EPS = 1e-5


def slot_ids(route_dev, experts, local_experts, capacity):
    expert_ids = jnp.arange(experts, dtype=jnp.int32)
    first_hot = (route_dev[:, 0:1] == expert_ids).astype(jnp.int32)
    second_hot = (route_dev[:, 1:2] == expert_ids).astype(jnp.int32)
    first_run = jnp.cumsum(first_hot, axis=0)
    second_run = jnp.cumsum(second_hot, axis=0) + first_run[-1:, :]
    first_pos = jnp.sum((first_run - 1) * first_hot, axis=-1)
    second_pos = jnp.sum((second_run - 1) * second_hot, axis=-1)

    def slot(ids, pos):
        rank = (ids % local_experts) * (experts // local_experts) + ids // local_experts
        return jnp.where(pos < capacity, rank * capacity + pos, -1)

    return slot(route_dev[:, 0], first_pos), slot(route_dev[:, 1], second_pos)


def solution(mesh):
    ep_size = mesh.shape['ep']
    token_spec = P(('dp', 'ep'), None)
    expert_spec = P('ep', None, None)
    lead_dims = (((0,), (0,)), ((), ()))
    f32, bf16 = jnp.float32, jnp.bfloat16

    def reduce_over_dp(grad):
        part = lax.psum_scatter(grad, 'dp', scatter_dimension=0, tiled=True)
        return lax.all_gather(part.astype(bf16), 'dp', axis=0, tiled=True)

    def local_step(tokens, out_grad, routes, norm_gain, w_router, w_gate, w_up, w_down):
        tok_count, model_width = tokens.shape
        local_experts = w_gate.shape[0]
        experts = local_experts * ep_size
        capacity = (CAPACITY_NUM * tok_count * 2 + CAPACITY_DEN * experts - 1) // (CAPACITY_DEN * experts)
        held = ep_size * capacity
        first_slot, second_slot = slot_ids(routes, experts, local_experts, capacity)
        route_hot = (routes[:, :, None] == jnp.arange(experts, dtype=jnp.int32)).astype(f32)

        def maps(start, count):
            ids = start + jnp.arange(count, dtype=jnp.int32)
            return (first_slot[:, None] == ids).astype(bf16), (second_slot[:, None] == ids).astype(bf16)

        x_f32 = tokens.astype(f32)
        inv_rms = lax.rsqrt(jnp.mean(x_f32 * x_f32, axis=-1, keepdims=True) + NORM_EPS)
        unit_rows = x_f32 * inv_rms
        normed = (unit_rows * norm_gain).astype(bf16)
        logits = jnp.dot(normed, w_router, preferred_element_type=f32)
        gate_probs = jax.nn.softmax(jnp.einsum('te,tke->tk', logits, route_hot), axis=-1)
        dy_f32 = out_grad.astype(f32)
        first_dy = (gate_probs[:, 0:1] * dy_f32).astype(bf16)
        second_dy = (gate_probs[:, 1:2] * dy_f32).astype(bf16)

        recv, d_out = [], []
        for j in range(local_experts):
            first_map, second_map = maps(j * held, held)
            rows = lax.dot_general(first_map + second_map, normed, lead_dims, preferred_element_type=f32).astype(bf16)
            d_rows = (lax.dot_general(first_map, first_dy, lead_dims, preferred_element_type=f32)
                      + lax.dot_general(second_map, second_dy, lead_dims, preferred_element_type=f32)).astype(bf16)
            recv.append(lax.all_to_all(rows.reshape(ep_size, capacity, model_width), 'ep', 0, 0).reshape(held, model_width))
            d_out.append(lax.all_to_all(d_rows.reshape(ep_size, capacity, model_width), 'ep', 0, 0).reshape(held, model_width))

        saved, grads = [], []
        for j in range(local_experts):
            u, dv = recv[j], d_out[j]
            gate_act = jnp.dot(u, w_gate[j], preferred_element_type=f32)
            up_act = jnp.dot(u, w_up[j], preferred_element_type=f32)
            silu_gate = jax.nn.silu(gate_act)
            hidden = (silu_gate * up_act).astype(bf16)
            grad_down = lax.dot_general(hidden, dv, lead_dims, preferred_element_type=f32)
            d_hidden = lax.dot_general(dv, w_down[j], (((1,), (1,)), ((), ())), preferred_element_type=f32)
            sig_gate = jax.nn.sigmoid(gate_act)
            d_gate_act = (d_hidden * up_act * sig_gate * (1.0 + gate_act * (1.0 - sig_gate))).astype(bf16)
            d_up_act = (d_hidden * silu_gate).astype(bf16)
            grad_gate = lax.dot_general(u, d_gate_act, lead_dims, preferred_element_type=f32)
            grad_up = lax.dot_general(u, d_up_act, lead_dims, preferred_element_type=f32)
            saved.append((hidden, d_gate_act, d_up_act))
            grads.append((grad_down, grad_gate, grad_up))

        reduced = [[reduce_over_dp(g) for g in group] for group in grads]
        saved, _ = lax.optimization_barrier((saved, grads))
        y_rows, d_rows = [], []
        for j in range(local_experts):
            hidden, d_gate_act, d_up_act = saved[j]
            y_rows.append(jnp.dot(hidden, w_down[j], preferred_element_type=f32).astype(bf16))
            trans = (((1,), (1,)), ((), ()))
            d_rows.append((lax.dot_general(d_gate_act, w_gate[j], trans, preferred_element_type=f32)
                           + lax.dot_general(d_up_act, w_up[j], trans, preferred_element_type=f32)).astype(bf16))

        def send_back(rows):
            parts = [lax.all_to_all(r.reshape(ep_size, capacity, model_width), 'ep', 0, 0).reshape(held, model_width) for r in rows]
            return jnp.concatenate(parts, axis=0)

        back_rows = send_back(y_rows)
        d_back = send_back(d_rows)
        first_map, second_map = maps(0, local_experts * held)
        first_y = jnp.dot(first_map, back_rows, preferred_element_type=f32)
        second_y = jnp.dot(second_map, back_rows, preferred_element_type=f32)
        block_out = (x_f32 + gate_probs[:, 0:1] * first_y + gate_probs[:, 1:2] * second_y).astype(bf16)
        prob_grad = jnp.stack([jnp.sum(dy_f32 * first_y, axis=-1), jnp.sum(dy_f32 * second_y, axis=-1)], axis=-1)
        d_chosen = gate_probs * (prob_grad - jnp.sum(gate_probs * prob_grad, axis=-1, keepdims=True))
        d_logits = jnp.einsum('tk,tke->te', d_chosen, route_hot)
        d_normed = jnp.dot(first_map + second_map, d_back, preferred_element_type=f32)
        d_normed = d_normed + lax.dot_general(d_logits, w_router, (((1,), (1,)), ((), ())))
        grad_router = jnp.einsum('td,te->de', normed, d_logits, preferred_element_type=f32)
        grad_gain = jnp.sum(d_normed * unit_rows, axis=0)
        d_unit = d_normed * norm_gain
        tokens_grad = (dy_f32 + inv_rms * (d_unit - unit_rows * jnp.mean(d_unit * unit_rows, axis=-1, keepdims=True))).astype(bf16)

        def stacked(k):
            return jnp.stack([group[k] for group in reduced])

        return (block_out, tokens_grad,
                lax.psum(grad_gain, ('dp', 'ep')), lax.psum(grad_router, ('dp', 'ep')),
                stacked(1), stacked(2), stacked(0))

    return jax.shard_map(local_step, mesh=mesh,
                         in_specs=(token_spec, token_spec, token_spec, P(None), P(None, None), expert_spec, expert_spec, expert_spec),
                         out_specs=(token_spec, token_spec, P(None), P(None, None), expert_spec, expert_spec, expert_spec),
                         check_vma=False)
```
